32 devices in a mesh: aa: 4 (over x, core), ba: 8 (over z, y).
Axes of the slice: x: 2, y: 2, z: 4, core: 2. Of those that a mesh axis runs over, the one named last changes fastest.
Arguments:
- head_outputs: bfloat16 [1024, 4096], P('ba'), may hold values from -6 to 6
- stream: bfloat16 [1024, 4096], P('ba'), may hold values from -6 to 6
- adapter_down_factors: bfloat16 [4096, 512], P(None, 'aa'), may hold values from -0.09375 to 0.09375
- adapter_up_factors: bfloat16 [512, 4096], P('aa'), may hold values from -1.5 to 1.5
- norm_gain_vector: float32 [4096], replicated, may hold values from 0.5 to 1.5
- router_matrix: bfloat16 [4096, 8], replicated, may hold values from -0.09375 to 0.09375
- token_adapter_index: int32 [1024], P('ba'), may hold values from 0 to 31
- token_expert_index: int32 [1024, 2], P('ba'), may hold values from 0 to 7, all different within a row; in each aligned block of 128 rows (0 to 127, 128 to 255, ...) at most 48 rows name the same one
- gate_weight: bfloat16 [8, 4096, 14336], P('ba', None, 'aa'), may hold values from -0.09375 to 0.09375
- up_weight: bfloat16 [8, 4096, 14336], P('ba', None, 'aa'), may hold values from -0.09375 to 0.09375
- down_weight: bfloat16 [8, 14336, 4096], P('ba', 'aa'), may hold values from -0.046875 to 0.046875
Outputs:
- mixed: bfloat16 [1024, 4096], P('ba', 'aa')
- adapter_load: float32 [32], P('aa')
The draws below stay inside these ranges and needn't reach their ends.
Inputs may be any that keep to these rules, and one draw needn't show every extreme that they name: `token_expert_index`: the two experts of a row differ; in each aligned block of 128 rows no expert is named by more than 48 rows.
All inputs are finite; a program needn't handle non-finite values.
Results may differ from the reference program's by a relative error of at most 0.0049.
Values may be sent and summed in bfloat16 or wider, within the bound.
A program may use at most 192 MiB of HBM per device.

```python
import math
import jax
import jax.numpy as jnp
import numpy as np
from jax import lax

MODEL_DIM = 4096
FF = 14336
E = 8
ADAPTER_RANK = 16
TOK_DEV = 128
CAP = 48
TOKENS = 1024
ADAPTER_COUNT = 32
SLOTS = 8
SLOT_FF = 14336
N_BA = 8


def plant(drawn, stream_key, smallest, top_value):
    longest = drawn.shape.index(max(drawn.shape))
    spots = []
    for shift in (0, 1):
        where = [jax.random.randint(jax.random.fold_in(stream_key, axis), (), 0, length) for axis, length in enumerate(drawn.shape)]
        where[longest] = (where[longest] + shift) % drawn.shape[longest]
        spots.append(tuple(where))
    return drawn.at[spots[0]].set(smallest).at[spots[1]].set(top_value)


def shard_levels(rng, shape, split, smallest, high):
    factor_of = 1.0
    for dim, shards_of in split:
        heights = jax.random.uniform(jax.random.fold_in(jax.random.fold_in(rng, 6), dim), (shards_of,), jnp.float32, smallest / len(split), high / len(split))
        factor_of = factor_of * jnp.repeat(jnp.exp(heights), shape[dim] // shards_of).reshape((-1,) + (1,) * (len(shape) - 1 - dim))
    return factor_of


def rank_bounds(count, lean):
    loads = [(1 << 20) // math.isqrt(rank ** lean) + 1 for rank in range(1, count + 1)]
    deviation = 1 + sum(loads) // (1 << 30)
    return np.cumsum(np.array([max(1, weight // deviation) for weight in loads]))


def skewed_ids(own_key, extent, amount, slope):
    table = rank_bounds(amount, slope)
    lot = jax.random.randint(jax.random.fold_in(own_key, 1), extent, 0, int(table[amount - 1]))
    rank = jnp.searchsorted(jnp.asarray(table, jnp.int32), lot, side="right")
    return jax.random.permutation(jax.random.fold_in(own_key, 2), amount)[rank].astype(jnp.int32)


def deal_out(stream_key, own, number, rows, count, top, most, skew):
    sequence = jax.random.permutation(stream_key, count)
    heavy_load, ordinary = portions_of(count, rows * top, most, skew, True), portions_of(count, rows * top, most, skew, False)
    places = jnp.arange(count)

    def named(lengths, turn):
        used = int((lengths > 0).sum())
        fixed = max(1, used // 4)
        shifted = fixed + (places - fixed + turn * (used - fixed)) % max(1, count - fixed)
        return jnp.zeros((count,), jnp.int32).at[sequence[jnp.where(places < fixed, places, shifted)]].set(jnp.asarray(lengths, jnp.int32))

    lengths = jnp.where(number % 4 == 0, named(heavy_load, number // 4), named(ordinary, number - number // 4 - 1))
    mixed = jax.random.permutation(jax.random.fold_in(own, 3), count)
    giver, taker = mixed[0:count // 2 * 2:2], mixed[1:count // 2 * 2:2]
    margin = jnp.minimum(lengths[giver] - 1, most - lengths[taker]) // 2
    margin = jnp.where((giver == sequence[0]) | (taker == sequence[0]) | (lengths[taker] == 0), 0, jnp.maximum(margin, 0))
    shifted = jax.random.randint(jax.random.fold_in(own, 4), (count // 2,), 0, 1 << 20) % (margin + 1)
    lengths = lengths.at[giver].add(-shifted).at[taker].add(shifted)
    labels = jnp.searchsorted(jnp.cumsum(lengths), jnp.arange(rows * top), side="right").astype(jnp.int32)
    table = labels.reshape(top, rows).T
    table = table[jax.random.permutation(jax.random.fold_in(own, 1), rows)]
    turn = jax.random.randint(jax.random.fold_in(own, 2), (rows, 1), 0, top)
    return jnp.take_along_axis(table, (jnp.arange(top)[None, :] + turn) % top, axis=1)


def portions_of(amount, total, most, slope, full):
    portions = [(1 << 20) // math.isqrt(rank ** slope) + 1 for rank in range(1, amount + 1)]
    largest = most if full else min(most, max(-(-total // amount), total * portions[0] // sum(portions)))
    least = 1 if total - largest >= amount - 1 else 0
    counts, spare = [largest] + [least] * (amount - 1), total - largest - least * (amount - 1)
    while spare > 0:
        candidates = [i for i in range(1, amount) if counts[i] < largest] or [i for i in range(1, amount) if counts[i] < most]
        mass, remaining = sum([portions[i] for i in candidates]), spare
        for i in candidates:
            more = min(most - counts[i], max(1, remaining * portions[i] // mass), spare)
            counts[i] = counts[i] + more
            spare = spare - more
    return np.array(counts)


def bell_draw(key, extent, deviation, limit, shards=(), kind=jnp.bfloat16):
    values = jax.random.normal(key, extent, jnp.float32) * deviation
    if len(shards) > 0:
        values = shard_levels(key, extent, shards, -0.22, 0.18) * values
    return jnp.clip(values, min=-limit, max=limit).astype(kind)


def setup_inputs(seed: int = 0) -> dict:
    key_list = jax.random.split(jax.random.key(seed), 12)
    head_outputs = bell_draw(key_list[0], (TOKENS, MODEL_DIM), 1.0, 6.0, ((0, 8),))
    stream = bell_draw(key_list[1], (TOKENS, MODEL_DIM), 1.0, 6.0, ((0, 8),))
    adapter_down_factors = bell_draw(key_list[2], (MODEL_DIM, ADAPTER_COUNT * ADAPTER_RANK), MODEL_DIM ** -0.5, 0.09375, ((1, 4),))
    adapter_up_factors = bell_draw(key_list[3], (ADAPTER_COUNT * ADAPTER_RANK, MODEL_DIM), ADAPTER_RANK ** -0.5, 1.5, ((0, 4),))
    norm_gain_vector = jnp.clip(1.0 + 0.1 * jax.random.normal(key_list[4], (MODEL_DIM,), jnp.float32), 0.5, 1.5)
    router_matrix = bell_draw(key_list[5], (MODEL_DIM, E), MODEL_DIM ** -0.5, 0.09375)
    token_adapter_index = plant(skewed_ids(key_list[6], (TOKENS,), ADAPTER_COUNT, 2), jax.random.fold_in(key_list[6], 3), 0, ADAPTER_COUNT - 1).astype(jnp.int32)
    token_expert_index_keys = jax.random.split(jax.random.fold_in(key_list[7], 1), TOKENS // TOK_DEV)
    token_expert_index_turns = jax.random.permutation(jax.random.fold_in(key_list[7], 3), TOKENS // TOK_DEV)
    token_expert_index = jax.vmap(lambda own, number: deal_out(jax.random.fold_in(key_list[7], 2), own, number, TOK_DEV, E, 2, CAP, 2))(token_expert_index_keys, token_expert_index_turns).reshape((TOKENS, 2))
    gate_weight = bell_draw(key_list[8], (SLOTS, MODEL_DIM, SLOT_FF), MODEL_DIM ** -0.5, 0.09375, ((0, 8), (2, 4)))
    up_weight = bell_draw(key_list[9], (SLOTS, MODEL_DIM, SLOT_FF), MODEL_DIM ** -0.5, 0.09375, ((0, 8), (2, 4)))
    down_weight = bell_draw(key_list[10], (SLOTS, SLOT_FF, MODEL_DIM), FF ** -0.5, 0.046875, ((0, 8), (1, 4)))
    return dict(head_outputs=head_outputs, stream=stream, adapter_down_factors=adapter_down_factors, adapter_up_factors=adapter_up_factors, norm_gain_vector=norm_gain_vector, router_matrix=router_matrix, token_adapter_index=token_adapter_index, token_expert_index=token_expert_index, gate_weight=gate_weight, up_weight=up_weight, down_weight=down_weight)


EPS = 1e-05
ADAPTER_SCALE = 2.0

def reference(head_outputs, stream, adapter_down_factors, adapter_up_factors, norm_gain_vector, router_matrix, token_adapter_index, token_expert_index, gate_weight, up_weight, down_weight):
    rank_projected = jnp.dot(head_outputs, adapter_down_factors, preferred_element_type=jnp.float32)
    column_holder = jnp.arange(adapter_down_factors.shape[1], dtype=jnp.int32) // ADAPTER_RANK
    rank_projected = jnp.where(token_adapter_index[:, None] == column_holder[None, :], rank_projected, 0.0).astype(jnp.bfloat16)
    adapter_update = ADAPTER_SCALE * jnp.dot(rank_projected, adapter_up_factors, preferred_element_type=jnp.float32)
    residual_stream = stream.astype(jnp.float32) + adapter_update
    inv_norm = lax.rsqrt(lax.optimization_barrier(jnp.mean(residual_stream * residual_stream, axis=1, keepdims=True)) + EPS)
    normed = (residual_stream * inv_norm * norm_gain_vector).astype(jnp.bfloat16)
    logits = jnp.dot(normed, router_matrix, preferred_element_type=jnp.float32)
    picked = jnp.take_along_axis(logits, token_expert_index, axis=1)
    weights = 1.0 / (1.0 + jnp.exp(picked[:, ::-1] - picked))
    blocked = token_expert_index.reshape(N_BA, TOK_DEV * 2)
    expert_hits = (blocked[:, :, None] == jnp.arange(E, dtype=jnp.int32)[None, None, :]).astype(jnp.int32)
    before = jnp.cumsum(expert_hits, axis=1) - expert_hits
    position = lax.optimization_barrier(jnp.sum(before * expert_hits, axis=2))
    slot_index = (jnp.arange(N_BA, dtype=jnp.int32)[:, None] * CAP + position).reshape(-1)
    flat_experts = token_expert_index.reshape(-1)
    token_of = jnp.arange(TOKENS * 2, dtype=jnp.int32) // 2
    owner_tok = jnp.zeros((E, N_BA * CAP), jnp.int32).at[flat_experts, slot_index].set(token_of)
    halves = N_BA // E
    results = jnp.zeros((E, N_BA * CAP, normed.shape[1]), jnp.float32)
    for slot_number in range(N_BA):
        expert = slot_number // halves
        slot_rows = normed[owner_tok[expert]]
        gate_proj = jnp.dot(slot_rows, gate_weight[slot_number], preferred_element_type=jnp.float32)
        up_proj = jnp.dot(slot_rows, up_weight[slot_number], preferred_element_type=jnp.float32)
        hidden = (jax.nn.silu(gate_proj) * up_proj).astype(jnp.bfloat16)
        results = results.at[expert].add(jnp.dot(hidden, down_weight[slot_number], preferred_element_type=jnp.float32))
    expert_out = results[flat_experts, slot_index].reshape(TOKENS, 2, -1)
    mixed = residual_stream + lax.optimization_barrier(jnp.sum(weights[:, :, None] * expert_out, axis=1))
    adapter_load = lax.optimization_barrier(jnp.sum((token_adapter_index[:, None] == jnp.arange(ADAPTER_COUNT, dtype=jnp.int32)[None, :]).astype(jnp.float32), axis=0))
    return (mixed.astype(jnp.bfloat16), adapter_load)
```

```python
import functools

import jax
import jax.numpy as jnp
from jax import lax
from jax.experimental import pallas as pl
from jax.experimental.pallas import tpu as pltpu
from jax.sharding import PartitionSpec as P

E = 8
ADAPTER_RANK = 16
CAP = 48
CORES = 2
HALVES = 2

EPS = 1e-05
ADAPTER_SCALE = 2.0
GU_SLOTS = 3
DN_SLOTS = 2
MESH = pl.DeviceIdType.MESH
F32 = jnp.float32
BF16 = jnp.bfloat16
NT = (((1,), (1,)), ((), ()))


def cols(start, width):
    return pl.ds(pl.multiple_of(start, 128), width)


def remote(src, dst, sems, i, place):
    return pltpu.make_async_remote_copy(
        src_ref=src,
        dst_ref=dst,
        send_sem=sems[0].at[i],
        recv_sem=sems[1].at[i],
        device_id=place,
        device_id_type=MESH,
    )


def layer(
    n_aa, n_ba, nt,
    head_hbm, stream_hbm, down_hbm, up_hbm, gain_hbm, router_hbm, adapter_hbm, expert_hbm,
    gate_hbm, upw_hbm, dn_hbm,
    out_ref, load_ref,
    head, stream, down, up, gain, router, adapter, expert,
    up_all, low_all, sq_all, lg_all, ld_all, res, outgoing,
    x_all, gacc, uacc, hidden, gw, uw, dw,
    ys, c1, yown, xs, c2, bs, ret,
    in_s, gu_s, dn_s,
    up_s, up_r, low_s, low_r, sq_s, sq_r, lg_s, lg_r, ld_s, ld_r,
    z_s, z_r, x_s, x_r, c_s, c_r, f_s, f_r,
    p_s, p_r, q_s, q_r, b_s, b_r,
):
    aa, ba = lax.axis_index("aa"), lax.axis_index("ba")
    nx = n_aa // CORES
    x, core = aa // CORES, lax.rem(aa, CORES)
    partner = {"aa": x * CORES + 1 - core}
    toks = head.shape[0]
    held = down.shape[1]
    model_width = head.shape[1]
    width = model_width // n_aa
    half = width // HALVES
    ff = hidden.shape[1]
    ft = ff // nt
    rows = n_ba * CAP
    split = n_ba // E
    mine = cols(aa * width, width)
    lane = cols(core * half, half)
    aa_peers = [{"aa": lax.rem(aa + k, n_aa)} for k in range(1, n_aa)]
    ba_peers = [{"ba": lax.rem(ba + k, n_ba)} for k in range(1, n_ba)]
    x_peers = [{"aa": lax.rem(x + kx, nx) * CORES + core} for kx in range(1, nx)]
    sources = [lax.rem(ba - k + n_ba, n_ba) for k in range(n_ba)]
    targets = [lax.rem(ba + k, n_ba) for k in range(n_ba)]
    origins = [lax.rem(x - kx + nx, nx) for kx in range(nx)]

    barrier = pltpu.get_barrier_semaphore()
    greeted = aa_peers + ba_peers
    for place in greeted:
        pl.semaphore_signal(barrier, inc=1, device_id=place, device_id_type=MESH)

    pairs = [
        (up_hbm, up), (head_hbm, head), (down_hbm, down), (adapter_hbm, adapter),
        (expert_hbm, expert), (stream_hbm.at[:, mine], stream), (gain_hbm.at[:, mine], gain),
        (router_hbm.at[:, mine], router),
    ]
    loads = [pltpu.make_async_copy(src, dst, in_s.at[i]) for i, (src, dst) in enumerate(pairs)]
    for copy in loads:
        copy.start()

    iterations = HALVES * nx * nt

    def gu_copies(it):
        slot = lax.rem(it, GU_SLOTS)
        t, group = lax.rem(it, nt), lax.div(it, nt)
        h, kx = lax.div(group, nx), lax.rem(group, nx)
        block = lax.rem(x - kx + nx, nx)
        copies = []
        for c in range(CORES):
            top = pl.multiple_of((block * CORES + c) * width + h * half, half)
            for j, (src, dst) in enumerate(((gate_hbm, gw), (upw_hbm, uw))):
                copies.append(pltpu.make_async_copy(
                    src.at[0, pl.ds(top, half), cols(t * ft, ft)],
                    dst.at[slot, pl.ds(c * half, half), :],
                    gu_s.at[slot, c * 2 + j],
                ))
        return copies

    far_first = list(range(1, nx)) + [0]
    chunks = [(h, kx, side) for h in range(HALVES) for kx in far_first for side in (1, 0)]

    def dn_copy(d):
        h, kx, side = chunks[d]
        block = lax.rem(x + kx, nx) * CORES + (1 - core if side else core)
        slot = d % DN_SLOTS
        return pltpu.make_async_copy(
            dn_hbm.at[0, :, cols(block * width + h * half, half)], dw.at[slot], dn_s.at[slot]
        )

    pl.semaphore_wait(barrier, len(greeted))
    loads[0].wait()
    up_copies = []
    for k in range(1, n_aa):
        to = lax.rem(aa + k, n_aa)
        up_copies.append(remote(
            up.at[:, cols(to * width, width)], up_all.at[aa], (up_s, up_r), k - 1, {"aa": to}
        ))
    for copy in up_copies:
        copy.start()
    for copy in loads[1:4]:
        copy.wait()

    eye = (
        lax.broadcasted_iota(jnp.int32, (toks, toks), 0)
        == lax.broadcasted_iota(jnp.int32, (toks, toks), 1)
    )

    def column(row):
        return jnp.sum(jnp.where(eye, jnp.broadcast_to(row, (toks, toks)), 0.0), axis=1, keepdims=True)

    def as_row(col):
        return jnp.sum(jnp.where(eye, jnp.broadcast_to(col, (toks, toks)), 0.0), axis=0, keepdims=True)

    owner = column(adapter[...].astype(F32)).astype(jnp.int32)
    local = owner - aa * (held // ADAPTER_RANK)
    lanes = lax.broadcasted_iota(jnp.int32, (toks, held), 1)
    projected = jnp.dot(head[...], down[...], preferred_element_type=F32)
    low_all[aa] = jnp.where(local == lanes // ADAPTER_RANK, projected, 0.0).astype(BF16)
    low_copies = [
        remote(low_all.at[aa], low_all.at[aa], (low_s, low_r), i, p) for i, p in enumerate(aa_peers)
    ]
    for copy in low_copies:
        copy.start()
    tally = jnp.sum((local == lanes).astype(F32), axis=0, keepdims=True)
    ld_all[ba] = jnp.broadcast_to(tally, ld_all.shape[1:])
    ld_copies = [
        remote(ld_all.at[ba], ld_all.at[ba], (ld_s, ld_r), i, p) for i, p in enumerate(ba_peers)
    ]
    for copy in ld_copies:
        copy.start()
    for copy in loads[4:]:
        copy.wait()
    for it in range(min(GU_SLOTS, iterations)):
        for copy in gu_copies(it):
            copy.start()
    for d in range(DN_SLOTS):
        dn_copy(d).start()

    up_all[aa] = up[:, mine]
    gacc[...] = jnp.zeros(gacc.shape, F32)
    uacc[...] = jnp.zeros(uacc.shape, F32)
    first, second = expert[0:1, :], expert[1:2, :]
    experts = lax.broadcasted_iota(jnp.int32, (E, toks), 0)
    hit0, hit1 = (first == experts).astype(F32), (second == experts).astype(F32)
    hits = hit0 + hit1
    earlier = (
        lax.broadcasted_iota(jnp.int32, (toks, toks), 0)
        < lax.broadcasted_iota(jnp.int32, (toks, toks), 1)
    ).astype(F32)
    place = jnp.dot(hits.astype(BF16), earlier.astype(BF16), preferred_element_type=F32)
    marked = jnp.where(hits > 0.0, place, -1.0).astype(jnp.int32)
    spots = lax.broadcasted_iota(jnp.int32, (CAP, toks), 0)
    picks = jnp.concatenate(
        [(marked[e : e + 1, :] == spots).astype(F32).astype(BF16) for e in range(E)], axis=0
    )

    for copy in low_copies + up_copies:
        copy.wait_recv()
    delta = jnp.dot(low_all[0], up_all[0], preferred_element_type=F32)
    for j in range(1, n_aa):
        delta = delta + jnp.dot(low_all[j], up_all[j], preferred_element_type=F32)
    res[...] = stream[...].astype(F32) + ADAPTER_SCALE * delta
    square = as_row(jnp.sum(res[...] * res[...], axis=1, keepdims=True))
    sq_all[aa] = jnp.broadcast_to(square, sq_all.shape[1:])
    sq_copies = [
        remote(sq_all.at[aa], sq_all.at[aa], (sq_s, sq_r), i, p) for i, p in enumerate(aa_peers)
    ]
    for copy in sq_copies:
        copy.start()
    for copy in sq_copies:
        copy.wait_recv()
    total = sq_all[0]
    for j in range(1, n_aa):
        total = total + sq_all[j]
    inv_norm = column(lax.rsqrt(total[0:1, :] / model_width + EPS))
    normed = (res[...] * inv_norm * gain[...]).astype(BF16)

    def here(h, block):
        return h * nx + block

    def dispatch(h, k):
        return remote(
            outgoing.at[h, lax.div(targets[k], split)], x_all.at[here(h, x), ba, :, lane],
            (z_s, z_r), h * (n_ba - 1) + k - 1, {"ba": targets[k]},
        )

    for h in range(HALVES):
        sent = jnp.dot(picks, normed[:, h * half : (h + 1) * half], preferred_element_type=F32)
        outgoing[h] = sent.astype(BF16).reshape(E, CAP, half)
        for k in range(1, n_ba):
            dispatch(h, k).start()
        x_all[here(h, x), ba, :, lane] = outgoing[h, lax.div(ba, split)]

    lg_all[aa] = lax.dot_general(router[...], normed, NT, preferred_element_type=F32)
    lg_copies = [
        remote(lg_all.at[aa], lg_all.at[aa], (lg_s, lg_r), i, p) for i, p in enumerate(aa_peers)
    ]
    for copy in lg_copies:
        copy.start()

    def across(h, k, kx):
        block = x_all.at[here(h, x), sources[k], :, lane]
        i = (h * n_ba + k) * (nx - 1) + kx - 1
        return remote(block, block, (x_s, x_r), i, x_peers[kx - 1])

    def beside(h, k):
        block = x_all.at[here(h, x), sources[k], :, lane]
        return remote(block, block, (c_s, c_r), h * n_ba + k, partner)

    def passed(h, kx):
        block = x_all.at[here(h, origins[kx]), :, :, lane]
        return remote(block, block, (f_s, f_r), h * (nx - 1) + kx - 1, partner)

    def forward(h, k):
        if k:
            dispatch(h, k).wait_recv()
        for kx in range(1, nx):
            across(h, k, kx).start()
        beside(h, k).start()

    def settle(h):
        for k in range(n_ba):
            beside(h, k).wait_recv()

    def collect(h, kx):
        for k in range(n_ba):
            across(h, k, kx).wait_recv()
        passed(h, kx).start()

    per_half = nx * nt
    hooks = {}

    def hook(it, fn, *args):
        hooks.setdefault(it, []).append(functools.partial(fn, *args))

    for kx in range(1, nx):
        hook(max(1, kx * nt - 1), collect, 0, kx)
        hook(kx * nt, lambda kx: passed(0, kx).wait_recv(), kx)
    for k in range(n_ba):
        at = 1 + (0 if k < n_ba // 2 else (1 if k < 3 * n_ba // 4 else 2))
        hook(min(at, per_half - 1), forward, 1, k)
    hook(per_half, settle, 1)
    for kx in range(1, nx):
        hook(per_half + max(1, kx * nt - 1), collect, 1, kx)
        hook(per_half + kx * nt, lambda kx: passed(1, kx).wait_recv(), kx)

    def step(it, finish):
        for at, fns in hooks.items():
            if (at >= iterations - nt) == finish:
                @pl.when(it == at)
                def _():
                    for fn in fns:
                        fn()
        for copy in gu_copies(it):
            copy.wait()
        slot = lax.rem(it, GU_SLOTS)
        t, group = lax.rem(it, nt), lax.div(it, nt)
        h, kx = lax.div(group, nx), lax.rem(group, nx)
        lhs = x_all[here(h, lax.rem(x - kx + nx, nx))].reshape(rows, CORES * half)
        g = gacc[t] + jnp.dot(lhs, gw[slot], preferred_element_type=F32)
        u = uacc[t] + jnp.dot(lhs, uw[slot], preferred_element_type=F32)
        if finish:
            hidden[:, cols(t * ft, ft)] = (g / (1.0 + jnp.exp(-g)) * u).astype(BF16)
        else:
            gacc[t] = g
            uacc[t] = u

            @pl.when(it + GU_SLOTS < iterations)
            def _():
                for copy in gu_copies(it + GU_SLOTS):
                    copy.start()

    for k in range(n_ba):
        forward(0, k)
    settle(0)

    @pl.loop(0, iterations - nt)
    def _(it):
        step(it, False)

    @pl.loop(iterations - nt, iterations)
    def _(it):
        step(it, True)

    order = list(range(1, n_ba)) + [0]

    def to_partner(h, kx):
        return remote(ys.at[h, kx], c1.at[h, kx], (p_s, p_r), h * nx + kx, partner)

    def to_chip(h, kx, k):
        i = (h * (nx - 1) + kx - 1) * n_ba + k
        return remote(
            xs.at[h, kx - 1, targets[k]], c2.at[h, kx - 1, targets[k]], (q_s, q_r), i, x_peers[kx - 1]
        )

    def home(h, k):
        return remote(
            bs.at[h, k - 1], ret.at[h, ba], (b_s, b_r), h * (n_ba - 1) + k - 1, {"ba": targets[k]}
        )

    def give(h, k):
        to = targets[k]
        whole = yown[h, to]
        for kx in range(1, nx):
            to_chip(h, kx, k).wait_recv()
            whole = whole + c2[h, kx - 1, to].astype(F32)
        if k:
            bs[h, k - 1] = whole.astype(BF16)
            home(h, k).start()
        else:
            ret[h, ba] = whole.astype(BF16)

    gives = {}
    last = len(chunks) - 1
    ready = len(chunks) // HALVES - 1
    for n, k in enumerate(order):
        at = ready + (0, 0, 1, 2, 2, 3, 3, 4)[n * 8 // n_ba]
        gives.setdefault(min(at, last), []).append((0, k))
    for k in order:
        gives.setdefault(last, []).append((1, k))

    for d, (h, kx, side) in enumerate(chunks):
        dn_copy(d).wait()
        y = jnp.dot(hidden[...], dw[d % DN_SLOTS], preferred_element_type=F32)
        if side:
            ys[h, kx] = y.astype(BF16).reshape(n_ba, CAP, half)
            to_partner(h, kx).start()
        else:
            yown[h] = y.reshape(n_ba, CAP, half)
            to_partner(h, kx).wait_recv()
            if kx:
                for k in order:
                    to = targets[k]
                    xs[h, kx - 1, to] = (yown[h, to] + c1[h, kx, to].astype(F32)).astype(BF16)
                    to_chip(h, kx, k).start()
            else:
                yown[h] = yown[h] + c1[h, kx].astype(F32)
        if d + DN_SLOTS < len(chunks):
            dn_copy(d + DN_SLOTS).start()
        for hh, k in gives.get(d, []):
            give(hh, k)

    for copy in lg_copies + ld_copies:
        copy.wait_recv()
    logits = lg_all[0]
    for j in range(1, n_aa):
        logits = logits + lg_all[j]
    load = ld_all[0]
    for j in range(1, n_ba):
        load = load + ld_all[j]
    load_ref[...] = load
    own0 = jnp.sum(hit0 * logits, axis=0, keepdims=True)
    own1 = jnp.sum(hit1 * logits, axis=0, keepdims=True)
    weight0 = column(1.0 / (1.0 + jnp.exp(own1 - own0)))
    weight1 = column(1.0 / (1.0 + jnp.exp(own0 - own1)))
    seats = lax.broadcasted_iota(jnp.int32, (toks, rows), 1)

    def picked(which, hit):
        seat = which.astype(F32) * (split * CAP) + jnp.sum(hit * place, axis=0, keepdims=True)
        seat = column(seat).astype(jnp.int32)
        found = seats == seat
        for j in range(1, split):
            found = found | (seats == seat + j * CAP)
        return found.astype(F32).astype(BF16)

    pick0, pick1 = picked(first, hit0), picked(second, hit1)
    for h in range(HALVES):
        for k in range(1, n_ba):
            home(h, k).wait_recv()
        part = slice(h * half, (h + 1) * half)
        back = ret[h].reshape(rows, half)
        mixed = weight0 * jnp.dot(pick0, back, preferred_element_type=F32)
        mixed = mixed + weight1 * jnp.dot(pick1, back, preferred_element_type=F32)
        out_ref[:, part] = (res[:, part] + mixed).astype(BF16)

    for copy in up_copies + low_copies + sq_copies + lg_copies + ld_copies:
        copy.wait_send()
    for h in range(HALVES):
        for k in range(n_ba):
            if k:
                dispatch(h, k).wait_send()
                home(h, k).wait_send()
            beside(h, k).wait_send()
            for kx in range(1, nx):
                across(h, k, kx).wait_send()
                to_chip(h, kx, k).wait_send()
        for kx in range(nx):
            if kx:
                passed(h, kx).wait_send()
            to_partner(h, kx).wait_send()


def shards(
    head_outputs,
    stream,
    adapter_down_factors,
    adapter_up_factors,
    norm_gain_vector,
    router_matrix,
    token_adapter_index,
    token_expert_index,
    gate_weight,
    up_weight,
    down_weight,
):
    toks, model_width = head_outputs.shape
    n_aa, n_ba = lax.axis_size("aa"), lax.axis_size("ba")
    nx = n_aa // CORES
    held = adapter_down_factors.shape[1]
    ff = gate_weight.shape[2]
    width = model_width // n_aa
    half = width // HALVES
    rows = n_ba * CAP
    nt = 2 if ff % 512 == 0 else 1
    dma = pltpu.SemaphoreType.DMA
    vmem = pltpu.VMEM
    far = max(nx - 1, 1)

    def sems(n):
        return [dma((max(n, 1),)), dma((max(n, 1),))]

    mixed, load = pl.pallas_call(
        functools.partial(layer, n_aa, n_ba, nt),
        out_shape=(
            jax.ShapeDtypeStruct((toks, width), BF16),
            jax.ShapeDtypeStruct((8, held), F32),
        ),
        in_specs=[pl.BlockSpec(memory_space=pl.ANY)] * 11,
        out_specs=(pl.BlockSpec(memory_space=pltpu.VMEM),) * 2,
        scratch_shapes=[
            vmem((toks, model_width), BF16),
            vmem((toks, width), BF16),
            vmem((model_width, held), BF16),
            vmem((held, model_width), BF16),
            vmem((1, width), F32),
            vmem((E, width), BF16),
            vmem((1, toks), jnp.int32),
            vmem((2, toks), jnp.int32),
            vmem((n_aa, held, width), BF16),
            vmem((n_aa, toks, held), BF16),
            vmem((n_aa, 8, toks), F32),
            vmem((n_aa, E, toks), F32),
            vmem((n_ba, 8, held), F32),
            vmem((toks, width), F32),
            vmem((HALVES, E, CAP, half), BF16),
            vmem((HALVES * nx, n_ba, CAP, CORES * half), BF16),
            vmem((nt, rows, ff // nt), F32),
            vmem((nt, rows, ff // nt), F32),
            vmem((rows, ff), BF16),
            vmem((GU_SLOTS, CORES * half, ff // nt), BF16),
            vmem((GU_SLOTS, CORES * half, ff // nt), BF16),
            vmem((DN_SLOTS, ff, half), BF16),
            vmem((HALVES, nx, n_ba, CAP, half), BF16),
            vmem((HALVES, nx, n_ba, CAP, half), BF16),
            vmem((HALVES, n_ba, CAP, half), F32),
            vmem((HALVES, far, n_ba, CAP, half), BF16),
            vmem((HALVES, far, n_ba, CAP, half), BF16),
            vmem((HALVES, n_ba - 1, CAP, half), BF16),
            vmem((HALVES, n_ba, CAP, half), BF16),
            dma((8,)),
            dma((GU_SLOTS, 2 * CORES)),
            dma((DN_SLOTS,)),
        ]
        + sems(n_aa - 1) * 4
        + sems(n_ba - 1)
        + sems(HALVES * (n_ba - 1))
        + sems(HALVES * n_ba * (nx - 1))
        + sems(HALVES * n_ba)
        + sems(HALVES * (nx - 1))
        + sems(HALVES * nx)
        + sems(HALVES * n_ba * (nx - 1))
        + sems(HALVES * (n_ba - 1)),
        compiler_params=pltpu.CompilerParams(
            collective_id=0, has_side_effects=True, vmem_limit_bytes=67043328
        ),
        name="layer",
    )(
        head_outputs, stream, adapter_down_factors, adapter_up_factors,
        norm_gain_vector[None, :], router_matrix.T, token_adapter_index[None, :],
        token_expert_index.T, gate_weight, up_weight, down_weight,
    )
    return (mixed, load[0, : held // ADAPTER_RANK])


def solution(mesh):
    in_specs = (
        P("ba", None),
        P("ba", None),
        P(None, "aa"),
        P("aa", None),
        P(),
        P(),
        P("ba"),
        P("ba", None),
        P("ba", None, "aa"),
        P("ba", None, "aa"),
        P("ba", "aa", None),
    )
    out_specs = (P("ba", "aa"), P("aa"))
    return jax.shard_map(shards, mesh=mesh, in_specs=in_specs, out_specs=out_specs, check_vma=False)
```

```python
import functools

import jax
import jax.numpy as jnp
from jax import lax
from jax.experimental import pallas as pl
from jax.experimental.pallas import tpu as pltpu
from jax.sharding import PartitionSpec as P

E = 8
ADAPTER_RANK = 16
CAP = 48
CORES = 2
PARTS = 4

EPS = 1e-05
ADAPTER_SCALE = 2.0
GU_DEPTH = 3
DN_SLOTS = 2
MESH = pl.DeviceIdType.MESH
F32 = jnp.float32
BF16 = jnp.bfloat16
NT = (((1,), (1,)), ((), ()))


def cols(start, width):
    return pl.ds(pl.multiple_of(start, 128), width)


def remote(src, dst, sems, i, place):
    return pltpu.make_async_remote_copy(
        src_ref=src,
        dst_ref=dst,
        send_sem=sems[0].at[0],
        recv_sem=sems[1].at[i],
        device_id=place,
        device_id_type=MESH,
    )


def layer(
    n_aa, n_ba, nt,
    head_hbm, stream_hbm, down_hbm, up_hbm, gain_hbm, router_hbm, adapter_hbm, expert_hbm,
    gate_hbm, upw_hbm, dn_hbm,
    out_hbm, load_ref,
    head, stream, down, up, gain, router, adapter, expert,
    d_send, d_recv, e_send, e_recv, stat_all, note_all, ld_all, res, outgoing, scale,
    pick0, pick1, weight0, weight1, out,
    x_all, gacc, uacc, hidden, gw, uw, dw,
    ys, c1, yown, yfar, xs, c2, bs, ret,
    in_s, gu_s, dn_s, out_s,
    d_s, d_r, e_s, e_r, stat_s, stat_r, note_s, note_r, ld_s, ld_r,
    z_s, z_r, x_s, x_r, c_s, c_r, f_s, f_r,
    p_s, p_r, q_s, q_r, b_s, b_r,
):
    aa, ba = lax.axis_index("aa"), lax.axis_index("ba")
    nx = n_aa // CORES
    x, core = aa // CORES, lax.rem(aa, CORES)
    partner = {"aa": x * CORES + 1 - core}
    toks = head.shape[0]
    held = down.shape[1]
    model_width = head.shape[1]
    width = model_width // n_aa
    part = width // PARTS
    ff = hidden.shape[1]
    ft = ff // nt
    rows = n_ba * CAP
    split = n_ba // E
    mine = cols(aa * width, width)
    lane = cols(core * part, part)
    aa_peers = [{"aa": lax.rem(aa + k, n_aa)} for k in range(1, n_aa)]
    ba_peers = [{"ba": lax.rem(ba + k, n_ba)} for k in range(1, n_ba)]
    x_peers = [{"aa": lax.rem(x + kx, nx) * CORES + core} for kx in range(1, nx)]
    sources = [lax.rem(ba - k + n_ba, n_ba) for k in range(n_ba)]
    targets = [lax.rem(ba + k, n_ba) for k in range(n_ba)]
    origins = [lax.rem(x - kx + nx, nx) for kx in range(nx)]
    ahead = [lax.rem(x + kx, nx) for kx in range(nx)]
    far = list(range(1, nx))
    far_first = far + [0]

    barrier = pltpu.get_barrier_semaphore()
    greeted = aa_peers + ba_peers
    for place in greeted:
        pl.semaphore_signal(barrier, inc=1, device_id=place, device_id_type=MESH)

    pairs = [
        (head_hbm, head), (down_hbm, down), (adapter_hbm, adapter), (up_hbm, up),
        (expert_hbm, expert), (stream_hbm.at[:, mine], stream), (gain_hbm.at[:, mine], gain),
        (router_hbm.at[:, mine], router),
    ]
    loads = [pltpu.make_async_copy(src, dst, in_s.at[i]) for i, (src, dst) in enumerate(pairs)]
    for copy in loads:
        copy.start()

    groups = [(0, kx) for kx in range(nx)]
    for q in range(1, PARTS):
        groups += [(q, 0)] + ([(q - 1, kx) for kx in far] if q > 1 else [])
    groups += [(PARTS - 1, kx) for kx in far] if PARTS > 1 else []

    def gu_copies(n, t):
        q, kx = groups[n]
        slot = (n % GU_DEPTH) * nt + t
        copies = []
        for c in range(CORES):
            top = pl.multiple_of((origins[kx] * CORES + c) * width + q * part, part)
            for j, (src, dst) in enumerate(((gate_hbm, gw), (upw_hbm, uw))):
                copies.append(pltpu.make_async_copy(
                    src.at[0, pl.ds(top, part), cols(t * ft, ft)],
                    dst.at[slot, pl.ds(c * part, part), :],
                    gu_s.at[slot, j],
                ))
        return copies

    chunks = [(q, kx) for q in range(PARTS) for kx in far_first]

    def dn_copies(d):
        q, kx = chunks[d]
        slot = d % DN_SLOTS
        copies = []
        for side in range(CORES):
            block = ahead[kx] * CORES + (1 - core if side else core)
            copies.append(pltpu.make_async_copy(
                dn_hbm.at[0, :, cols(block * width + q * part, part)],
                dw.at[slot, side],
                dn_s.at[slot, side],
            ))
        return copies

    eye = (
        lax.broadcasted_iota(jnp.int32, (toks, toks), 0)
        == lax.broadcasted_iota(jnp.int32, (toks, toks), 1)
    )

    def column(row):
        return jnp.sum(jnp.where(eye, jnp.broadcast_to(row, (toks, toks)), 0.0), axis=1, keepdims=True)

    def as_row(col):
        return jnp.sum(jnp.where(eye, jnp.broadcast_to(col, (toks, toks)), 0.0), axis=0, keepdims=True)

    for copy in loads[:3]:
        copy.wait()
    owner = column(adapter[...].astype(F32)).astype(jnp.int32)
    local = owner - aa * (held // ADAPTER_RANK)
    lanes = lax.broadcasted_iota(jnp.int32, (toks, held), 1)
    projected = jnp.dot(head[...], down[...], preferred_element_type=F32)
    low = jnp.where(local == lanes // ADAPTER_RANK, projected, 0.0).astype(BF16)
    tally = jnp.sum((local == lanes).astype(F32), axis=0, keepdims=True)
    ld_all[ba] = jnp.broadcast_to(tally, ld_all.shape[1:])
    loads[3].wait()

    def term(q, kx, other):
        block = ahead[kx] * CORES + (1 - core if other else core)
        return jnp.dot(low, up[:, cols(block * width + q * part, part)], preferred_element_type=F32)

    def to_side(q, kx):
        return remote(d_send.at[q, kx], d_recv.at[q, kx], (d_s, d_r), q * nx + kx, partner)

    def to_far(q, kx):
        i = q * (nx - 1) + kx - 1
        return remote(e_send.at[q, kx - 1], e_recv.at[q, kx - 1], (e_s, e_r), i, x_peers[kx - 1])

    for q in range(PARTS):
        for kx in far_first:
            d_send[q, kx] = term(q, kx, True).astype(BF16)
    pl.semaphore_wait(barrier, len(greeted))
    for q in range(PARTS):
        for kx in far_first:
            to_side(q, kx).start()
    for copy in loads[4:]:
        copy.wait()
    for n in range(min(GU_DEPTH, len(groups))):
        for t in range(nt):
            for copy in gu_copies(n, t):
                copy.start()
    for d in range(DN_SLOTS):
        for copy in dn_copies(d):
            copy.start()
    ld_copies = [
        remote(ld_all.at[ba], ld_all.at[ba], (ld_s, ld_r), 0, p) for i, p in enumerate(ba_peers)
    ]
    for q in range(PARTS):
        for kx in far:
            own = term(q, kx, False)
            to_side(q, kx).wait_recv()
            e_send[q, kx - 1] = (own + d_recv[q, kx].astype(F32)).astype(BF16)
            to_far(q, kx).start()
    for copy in ld_copies:
        copy.start()

    first, second = expert[0:1, :], expert[1:2, :]
    experts = lax.broadcasted_iota(jnp.int32, (E, toks), 0)
    hit0, hit1 = (first == experts).astype(F32), (second == experts).astype(F32)
    hits = hit0 + hit1
    earlier = (
        lax.broadcasted_iota(jnp.int32, (toks, toks), 0)
        < lax.broadcasted_iota(jnp.int32, (toks, toks), 1)
    ).astype(F32)
    place = jnp.dot(hits.astype(BF16), earlier.astype(BF16), preferred_element_type=F32)
    marked = jnp.where(hits > 0.0, place, -1.0)
    spots = lax.broadcasted_iota(jnp.int32, (CAP, toks), 0)
    picks = jnp.concatenate(
        [(marked[e : e + 1, :].astype(jnp.int32) == spots).astype(F32).astype(BF16) for e in range(E)],
        axis=0,
    )
    seats = lax.broadcasted_iota(jnp.int32, (toks, rows), 1)

    def picked(which, hit):
        seat = which.astype(F32) * (split * CAP) + jnp.sum(hit * place, axis=0, keepdims=True)
        seat = column(seat).astype(jnp.int32)
        found = seats == seat
        for j in range(1, split):
            found = found | (seats == seat + j * CAP)
        return found.astype(F32).astype(BF16)

    pick0[...] = picked(first, hit0)
    pick1[...] = picked(second, hit1)

    def everyone(buf, sems):
        others = buf.at[pl.ds(0, buf.shape[0] - 1)]
        return remote(others, others, sems, 0, partner)

    def here(q, block):
        return q * nx + block

    def dispatch(q, k):
        return remote(
            outgoing.at[q, lax.div(targets[k], split)], x_all.at[here(q, x), ba, :, lane],
            (z_s, z_r), q * (n_ba - 1) + k - 1, {"ba": targets[k]},
        )

    square = jnp.zeros((toks, 1), F32)
    votes = jnp.zeros((E, toks), F32)
    for q in range(PARTS):
        where = slice(q * part, (q + 1) * part)
        delta = term(q, 0, False)
        to_side(q, 0).wait_recv()
        delta = delta + d_recv[q, 0].astype(F32)
        for kx in far:
            to_far(q, kx).wait_recv()
            delta = delta + e_recv[q, kx - 1].astype(F32)
        residual = stream[:, where].astype(F32) + ADAPTER_SCALE * delta
        res[:, where] = residual
        gained = (residual * gain[:, where]).astype(BF16)
        sent = jnp.dot(picks, gained, preferred_element_type=F32)
        outgoing[q] = sent.astype(BF16).reshape(E, CAP, part)
        for k in range(1, n_ba):
            dispatch(q, k).start()
        x_all[here(q, x), ba, :, lane] = outgoing[q, lax.div(ba, split)]
        square = square + jnp.sum(residual * residual, axis=1, keepdims=True)
        votes = votes + lax.dot_general(router[:, where], gained, NT, preferred_element_type=F32)
    stat_all[aa, 0:E] = votes
    stat_all[aa, E : 2 * E] = jnp.broadcast_to(as_row(square), (E, toks))
    stat_copies = [
        remote(stat_all.at[aa], stat_all.at[aa], (stat_s, stat_r), 0, p) for i, p in enumerate(aa_peers)
    ]
    for copy in stat_copies:
        copy.start()
    note_copies = [
        remote(note_all.at[ba], note_all.at[ba], (note_s, note_r), 0, p) for i, p in enumerate(ba_peers)
    ]

    def weigh():
        everyone(stat_all, (stat_s, stat_r)).wait_recv()
        stats = stat_all[0]
        for j in range(1, n_aa):
            stats = stats + stat_all[j]
        inv = lax.rsqrt(stats[E : 2 * E, :] / model_width + EPS)
        note_all[ba, 0:E] = marked
        note_all[ba, E : 2 * E] = inv
        for copy in note_copies:
            copy.start()
        logits = stats[0:E, :] * inv
        own0 = jnp.sum(hit0 * logits, axis=0, keepdims=True)
        own1 = jnp.sum(hit1 * logits, axis=0, keepdims=True)
        weight0[...] = jnp.broadcast_to(column(1.0 / (1.0 + jnp.exp(own1 - own0))), weight0.shape)
        weight1[...] = jnp.broadcast_to(column(1.0 / (1.0 + jnp.exp(own0 - own1))), weight1.shape)

    def read_notes():
        everyone(note_all, (note_s, note_r)).wait_recv()
        everyone(ld_all, (ld_s, ld_r)).wait_recv()
        load = ld_all[0]
        for j in range(1, n_ba):
            load = load + ld_all[j]
        load_ref[...] = load[0:1, 0 : load_ref.shape[1]]
        for s in range(n_ba):
            note = note_all[s, pl.ds(lax.div(ba, split), 1), :]
            seen = note.astype(jnp.int32) == spots
            inv = jnp.sum(jnp.where(seen, note_all[s, E : E + 1, :], 0.0), axis=1, keepdims=True)
            scale[s * CAP : (s + 1) * CAP, :] = jnp.broadcast_to(inv, (CAP, scale.shape[1]))

    def across(q, k, kx):
        block = x_all.at[here(q, x), sources[k], :, lane]
        return remote(block, block, (x_s, x_r), q * (nx - 1) + kx - 1, x_peers[kx - 1])

    def beside(q, k):
        block = x_all.at[here(q, x), sources[k], :, lane]
        return remote(block, block, (c_s, c_r), q, partner)

    def passed(q, kx):
        block = x_all.at[here(q, origins[kx]), :, :, lane]
        return remote(block, block, (f_s, f_r), q * (nx - 1) + kx - 1, partner)

    arrival = list(range(n_ba))

    def forward(q, k):
        if k:
            dispatch(q, k).wait_recv()
        for kx in far:
            across(q, k, kx).start()
        beside(q, k).start()

    def collect(q, kx):
        block = x_all.at[here(q, origins[kx]), :, :, lane]
        i = q * (nx - 1) + kx - 1
        remote(block, block, (x_s, x_r), i, x_peers[kx - 1]).wait_recv()
        passed(q, kx).start()

    steps = len(groups) * nt
    hooks = {}

    def hook(it, fn, *args):
        hooks.setdefault(min(it, steps - 1), []).append(functools.partial(fn, *args))

    def whole(it):
        return -(-it // nt) * nt if it > 3 * nt else it

    for q in range(1, PARTS):
        need = groups.index((q, 0)) * nt
        for n, k in enumerate(arrival):
            due = -(-(264 * (q - 1) + 264 * (n + 1) // n_ba + 60) // 100) * nt // 2
            hook(whole(min(max(due, 1), need)), forward, q, k)
    for q in range(PARTS):
        for kx in far:
            need = groups.index((q, kx)) * nt
            floor = groups.index((q, 0)) * nt + (1 if q == 0 else nt)
            hook(max(need - (nt if q else 1), min(floor, need)), collect, q, kx)
    hook((len(groups) - 2) * nt, read_notes)

    def ready(n):
        q, kx = groups[n]
        if kx:
            passed(q, kx).wait_recv()
        else:
            block = x_all.at[here(q, x), :, :, lane]
            remote(block, block, (c_s, c_r), q, partner).wait_recv()

    for k in arrival:
        forward(0, k)
    weigh()
    for n, (q, kx) in enumerate(groups):
        for fn in hooks.get(n * nt, []):
            fn()
        ready(n)

        def fetched(t):
            slot = (n % GU_DEPTH) * nt + t
            for j, buf in enumerate((gw, uw)):
                pltpu.make_async_copy(buf.at[slot], buf.at[slot], gu_s.at[slot, j]).wait()

        def tile(t):
            slot = (n % GU_DEPTH) * nt + t
            lhs = x_all[here(q, origins[kx])].reshape(rows, CORES * part)
            g = jnp.dot(lhs, gw[slot], preferred_element_type=F32)
            u = jnp.dot(lhs, uw[slot], preferred_element_type=F32)
            if n:
                g = gacc[t] + g
                u = uacc[t] + u
            if n == len(groups) - 1:
                factor = scale[:, 0:1]
                g = g * factor
                hidden[:, cols(t * ft, ft)] = (g / (1.0 + jnp.exp(-g)) * (u * factor)).astype(BF16)
            else:
                gacc[t] = g
                uacc[t] = u

        def refill(t):
            if n + GU_DEPTH < len(groups):
                for copy in gu_copies(n + GU_DEPTH, t):
                    copy.start()

        between = [hooks.get(n * nt + j, []) for j in range(1, nt)]
        if nt == 2 and not any(between):
            for stage in (fetched, tile, refill):
                for t in range(nt):
                    stage(t)
        else:
            @pl.loop(0, nt)
            def _(t):
                for j, fns in enumerate(between):
                    if fns:
                        @pl.when(t == j + 1)
                        def _():
                            for fn in fns:
                                fn()
                fetched(t)
                tile(t)
                refill(t)

    def to_partner(q, kx):
        return remote(ys.at[q, kx], c1.at[q, kx], (p_s, p_r), q * nx + kx, partner)

    def to_chip(q, kx, k):
        i = (q * (nx - 1) + kx - 1) * n_ba + k
        return remote(
            xs.at[q, kx - 1, targets[k]], c2.at[q, kx - 1, targets[k]], (q_s, q_r), i, x_peers[kx - 1]
        )

    def home(q, k):
        return remote(
            bs.at[q, k - 1], ret.at[q, ba], (b_s, b_r), q, {"ba": targets[k]}
        )

    def give(q, k):
        to = targets[k]
        whole = yown[q, to]
        for kx in far:
            to_chip(q, kx, k).wait_recv()
            whole = whole + c2[q, kx - 1, to].astype(F32)
        if k:
            bs[q, k - 1] = whole.astype(BF16)
            home(q, k).start()
        else:
            ret[q, ba] = whole.astype(BF16)

    def leave(q):
        where = pl.ds(q * part, part)
        return pltpu.make_async_copy(out.at[:, where], out_hbm.at[:, where], out_s.at[q])

    def blend(q):
        remote(bs.at[q], bs.at[q], (b_s, b_r), q, partner).wait_recv()
        where = slice(q * part, (q + 1) * part)
        back = ret[q].reshape(rows, part)
        mixed = weight0[:, 0:1] * jnp.dot(pick0[...], back, preferred_element_type=F32)
        mixed = mixed + weight1[:, 0:1] * jnp.dot(pick1[...], back, preferred_element_type=F32)
        out[:, where] = (res[:, where] + mixed).astype(BF16)
        leave(q).start()

    order = list(range(1, n_ba)) + [0]
    last = len(chunks) - 1
    gives = {}
    for q in range(PARTS):
        for n, k in enumerate(order):
            due = -(-(540 + 420 * q + 52 * n * 8 // n_ba) // 160) - 1
            due = max(due * nx // 2, (q + 1) * nx)
            gives.setdefault(min(due, last), []).append((q, k))

    def finish(q, kx):
        to_partner(q, kx).wait_recv()
        if kx:
            for k in order:
                to = targets[k]
                xs[q, kx - 1, to] = (yfar[kx - 1, to] + c1[q, kx, to].astype(F32)).astype(BF16)
                to_chip(q, kx, k).start()
        else:
            yown[q] = yown[q] + c1[q, kx].astype(F32)

    late = None
    for d, (q, kx) in enumerate(chunks):
        for copy in dn_copies(d):
            copy.wait()
        slot = d % DN_SLOTS
        y = [jnp.dot(hidden[...], dw[slot, i], preferred_element_type=F32) for i in range(CORES)]
        ys[q, kx] = y[1].astype(BF16).reshape(n_ba, CAP, part)
        to_partner(q, kx).start()
        if kx:
            yfar[kx - 1] = y[0].reshape(n_ba, CAP, part)
        else:
            yown[q] = y[0].reshape(n_ba, CAP, part)
        if d + DN_SLOTS < len(chunks):
            for copy in dn_copies(d + DN_SLOTS):
                copy.start()
        if late is not None:
            finish(*late)
        late = (q, kx)
        if d == 0 or d == last:
            finish(q, kx)
            late = None
        done = set()
        for qq, k in gives.get(d, []):
            if d == last and qq > 1 and qq - 2 not in done:
                blend(qq - 2)
                done.add(qq - 2)
            give(qq, k)
    for q in range(PARTS):
        if q not in done:
            blend(q)

    for buf, sems in ((stat_all, (stat_s, stat_r)), (note_all, (note_s, note_r)), (ld_all, (ld_s, ld_r))):
        everyone(buf, sems).wait_send()
    local_part = x_all.at[pl.ds(0, PARTS), :, :, pl.ds(0, part)]
    passes = x_all.at[pl.ds(0, PARTS * (nx - 1)), :, :, pl.ds(0, part)]
    for buf, sems in (
        (bs, (z_s, z_r)), (bs, (b_s, b_r)), (local_part, (c_s, c_r)), (passes, (x_s, x_r)),
        (passes, (f_s, f_r)), (xs, (q_s, q_r)), (ys, (p_s, p_r)), (d_send, (d_s, d_r)),
        (e_send, (e_s, e_r)),
    ):
        remote(buf, buf, sems, 0, partner).wait_send()
    for q in range(PARTS):
        leave(q).wait()


def shards(
    head_outputs,
    stream,
    adapter_down_factors,
    adapter_up_factors,
    norm_gain_vector,
    router_matrix,
    token_adapter_index,
    token_expert_index,
    gate_weight,
    up_weight,
    down_weight,
):
    toks, model_width = head_outputs.shape
    n_aa, n_ba = lax.axis_size("aa"), lax.axis_size("ba")
    nx = n_aa // CORES
    held = adapter_down_factors.shape[1]
    ff = gate_weight.shape[2]
    width = model_width // n_aa
    part = width // PARTS
    rows = n_ba * CAP
    nt = 2 if ff % 512 == 0 else ff // 128
    dma = pltpu.SemaphoreType.DMA
    vmem = pltpu.VMEM
    far = max(nx - 1, 1)

    def sems(n):
        return [dma((1,)), dma((max(n, 1),))]

    mixed, load = pl.pallas_call(
        functools.partial(layer, n_aa, n_ba, nt),
        out_shape=(
            jax.ShapeDtypeStruct((toks, width), BF16),
            jax.ShapeDtypeStruct((1, held // ADAPTER_RANK), F32),
        ),
        in_specs=[pl.BlockSpec(memory_space=pl.ANY)] * 11,
        out_specs=(pl.BlockSpec(memory_space=pl.ANY), pl.BlockSpec(memory_space=pltpu.VMEM)),
        scratch_shapes=[
            vmem((toks, model_width), BF16),
            vmem((toks, width), BF16),
            vmem((model_width, held), BF16),
            vmem((held, model_width), BF16),
            vmem((1, width), F32),
            vmem((E, width), BF16),
            vmem((1, toks), jnp.int32),
            vmem((2, toks), jnp.int32),
            vmem((PARTS, nx, toks, part), BF16),
            vmem((PARTS, nx, toks, part), BF16),
            vmem((PARTS, far, toks, part), BF16),
            vmem((PARTS, far, toks, part), BF16),
            vmem((n_aa, 2 * E, toks), F32),
            vmem((n_ba, 2 * E, toks), F32),
            vmem((n_ba, 8, held), F32),
            vmem((toks, width), F32),
            vmem((PARTS, E, CAP, part), BF16),
            vmem((rows, 128), F32),
            vmem((toks, rows), BF16),
            vmem((toks, rows), BF16),
            vmem((toks, 128), F32),
            vmem((toks, 128), F32),
            vmem((toks, width), BF16),
            vmem((PARTS * nx, n_ba, CAP, CORES * part), BF16),
            vmem((nt, rows, ff // nt), F32),
            vmem((nt, rows, ff // nt), F32),
            vmem((rows, ff), BF16),
            vmem((GU_DEPTH * nt, CORES * part, ff // nt), BF16),
            vmem((GU_DEPTH * nt, CORES * part, ff // nt), BF16),
            vmem((DN_SLOTS, CORES, ff, part), BF16),
            vmem((PARTS, nx, n_ba, CAP, part), BF16),
            vmem((PARTS, nx, n_ba, CAP, part), BF16),
            vmem((PARTS, n_ba, CAP, part), F32),
            vmem((far, n_ba, CAP, part), F32),
            vmem((PARTS, far, n_ba, CAP, part), BF16),
            vmem((PARTS, far, n_ba, CAP, part), BF16),
            vmem((PARTS, n_ba - 1, CAP, part), BF16),
            vmem((PARTS, n_ba, CAP, part), BF16),
            dma((8,)),
            dma((GU_DEPTH * nt, 2)),
            dma((DN_SLOTS, CORES)),
            dma((PARTS,)),
        ]
        + sems(PARTS * nx)
        + sems(PARTS * (nx - 1))
        + sems(1) * 3
        + sems(PARTS * (n_ba - 1))
        + sems(PARTS * (nx - 1))
        + sems(PARTS)
        + sems(PARTS * (nx - 1))
        + sems(PARTS * nx)
        + sems(PARTS * n_ba * (nx - 1))
        + sems(PARTS),
        compiler_params=pltpu.CompilerParams(
            collective_id=0, has_side_effects=True, vmem_limit_bytes=67043328
        ),
        name="layer",
    )(
        head_outputs, stream, adapter_down_factors, adapter_up_factors,
        norm_gain_vector[None, :], router_matrix.T, token_adapter_index[None, :],
        token_expert_index.T, gate_weight, up_weight, down_weight,
    )
    return (mixed, load.reshape(held // ADAPTER_RANK))


def solution(mesh):
    in_specs = (
        P("ba", None),
        P("ba", None),
        P(None, "aa"),
        P("aa", None),
        P(),
        P(),
        P("ba"),
        P("ba", None),
        P("ba", None, "aa"),
        P("ba", None, "aa"),
        P("ba", "aa", None),
    )
    out_specs = (P("ba", "aa"), P("aa"))
    return jax.shard_map(shards, mesh=mesh, in_specs=in_specs, out_specs=out_specs, check_vma=False)
```

```python
import functools

import jax
import jax.numpy as jnp
from jax import lax
from jax.experimental import pallas as pl
from jax.experimental.pallas import tpu as pltpu
from jax.sharding import PartitionSpec as P

E = 8
ADAPTER_RANK = 16
CAP = 48
CORES = 2
PARTS = 4

EPS = 1e-05
ADAPTER_SCALE = 2.0
GU_DEPTH = 3
DN_SLOTS = 2
MESH = pl.DeviceIdType.MESH
F32 = jnp.float32
BF16 = jnp.bfloat16
NT = (((1,), (1,)), ((), ()))


def cols(start, width):
    return pl.ds(pl.multiple_of(start, 128), width)


def remote(src, dst, sems, i, place):
    return pltpu.make_async_remote_copy(
        src_ref=src,
        dst_ref=dst,
        send_sem=sems[0].at[0],
        recv_sem=sems[1].at[i],
        device_id=place,
        device_id_type=MESH,
    )


def layer(
    n_aa, n_ba, nt,
    head_hbm, stream_hbm, down_hbm, up_hbm, gain_hbm, router_hbm, adapter_hbm, expert_hbm,
    gate_hbm, upw_hbm, dn_hbm,
    out_hbm, load_ref,
    head, stream, down, up, gain, router, adapter, expert,
    d_send, d_recv, e_send, e_recv, stat_all, note_all, ld_all, res, outgoing, scale,
    pick0, pick1, weight0, weight1, out,
    x_all, gacc, uacc, hidden, gw, uw, dw,
    ys, c1, yown, yfar, xs, c2, bs, ret,
    in_s, gu_s, dn_s, out_s,
    d_s, d_r, e_s, e_r, stat_s, stat_r, note_s, note_r, ld_s, ld_r,
    z_s, z_r, x_s, x_r, c_s, c_r, f_s, f_r,
    p_s, p_r, q_s, q_r, b_s, b_r,
):
    aa, ba = lax.axis_index("aa"), lax.axis_index("ba")
    nx = n_aa // CORES
    x, core = aa // CORES, lax.rem(aa, CORES)
    partner = {"aa": x * CORES + 1 - core}
    toks = head.shape[0]
    held = down.shape[1]
    model_width = head.shape[1]
    width = model_width // n_aa
    part = width // PARTS
    ff = hidden.shape[1]
    ft = ff // nt
    rows = n_ba * CAP
    split = n_ba // E
    mine = cols(aa * width, width)
    lane = cols(core * part, part)
    aa_peers = [{"aa": lax.rem(aa + k, n_aa)} for k in range(1, n_aa)]
    ba_peers = [{"ba": lax.rem(ba + k, n_ba)} for k in range(1, n_ba)]
    x_peers = [{"aa": lax.rem(x + kx, nx) * CORES + core} for kx in range(1, nx)]
    sources = [lax.rem(ba - k + n_ba, n_ba) for k in range(n_ba)]
    targets = [lax.rem(ba + k, n_ba) for k in range(n_ba)]
    origins = [lax.rem(x - kx + nx, nx) for kx in range(nx)]
    ahead = [lax.rem(x + kx, nx) for kx in range(nx)]
    far = list(range(1, nx))
    far_first = far + [0]

    barrier = pltpu.get_barrier_semaphore()
    greeted = aa_peers + ba_peers
    for place in greeted:
        pl.semaphore_signal(barrier, inc=1, device_id=place, device_id_type=MESH)

    pairs = [
        (head_hbm, head), (down_hbm, down), (adapter_hbm, adapter), (up_hbm, up),
        (expert_hbm, expert), (stream_hbm.at[:, mine], stream), (gain_hbm.at[:, mine], gain),
        (router_hbm.at[:, mine], router),
    ]
    loads = [pltpu.make_async_copy(src, dst, in_s.at[i]) for i, (src, dst) in enumerate(pairs)]
    for copy in loads:
        copy.start()

    groups = [(0, kx) for kx in range(nx)]
    for q in range(1, PARTS):
        groups += [(q, 0)] + ([(q - 1, kx) for kx in far] if q > 1 else [])
    groups += [(PARTS - 1, kx) for kx in far] if PARTS > 1 else []

    def gu_copies(n, t):
        q, kx = groups[n]
        slot = (n % GU_DEPTH) * nt + t
        copies = []
        for c in range(CORES):
            top = pl.multiple_of((origins[kx] * CORES + c) * width + q * part, part)
            for j, (src, dst) in enumerate(((gate_hbm, gw), (upw_hbm, uw))):
                copies.append(pltpu.make_async_copy(
                    src.at[0, pl.ds(top, part), cols(t * ft, ft)],
                    dst.at[slot, pl.ds(c * part, part), :],
                    gu_s.at[slot, j],
                ))
        return copies

    chunks = [(q, kx) for q in range(PARTS) for kx in far_first]

    def dn_copies(d):
        q, kx = chunks[d]
        slot = d % DN_SLOTS
        copies = []
        for side in range(CORES):
            block = ahead[kx] * CORES + (1 - core if side else core)
            copies.append(pltpu.make_async_copy(
                dn_hbm.at[0, :, cols(block * width + q * part, part)],
                dw.at[slot, side],
                dn_s.at[slot, side],
            ))
        return copies

    eye = (
        lax.broadcasted_iota(jnp.int32, (toks, toks), 0)
        == lax.broadcasted_iota(jnp.int32, (toks, toks), 1)
    )

    def column(row):
        return jnp.sum(jnp.where(eye, jnp.broadcast_to(row, (toks, toks)), 0.0), axis=1, keepdims=True)

    def as_row(col):
        return jnp.sum(jnp.where(eye, jnp.broadcast_to(col, (toks, toks)), 0.0), axis=0, keepdims=True)

    for copy in loads[:3]:
        copy.wait()
    owner = column(adapter[...].astype(F32)).astype(jnp.int32)
    local = owner - aa * (held // ADAPTER_RANK)
    lanes = lax.broadcasted_iota(jnp.int32, (toks, held), 1)
    projected = jnp.dot(head[...], down[...], preferred_element_type=F32)
    low = jnp.where(local == lanes // ADAPTER_RANK, projected, 0.0).astype(BF16)
    tally = jnp.sum((local == lanes).astype(F32), axis=0, keepdims=True)
    ld_all[ba] = jnp.broadcast_to(tally, ld_all.shape[1:])
    loads[3].wait()

    def term(q, kx, other):
        block = ahead[kx] * CORES + (1 - core if other else core)
        return jnp.dot(low, up[:, cols(block * width + q * part, part)], preferred_element_type=F32)

    def to_side(q, kx):
        return remote(d_send.at[q, kx], d_recv.at[q, kx], (d_s, d_r), q * nx + kx, partner)

    def to_far(q, kx):
        i = q * (nx - 1) + kx - 1
        return remote(e_send.at[q, kx - 1], e_recv.at[q, kx - 1], (e_s, e_r), i, x_peers[kx - 1])

    for q in range(PARTS):
        for kx in far_first:
            d_send[q, kx] = term(q, kx, True).astype(BF16)
    pl.semaphore_wait(barrier, len(greeted))
    for q in range(PARTS):
        for kx in far_first:
            to_side(q, kx).start()
    for copy in loads[4:]:
        copy.wait()
    for n in range(min(GU_DEPTH, len(groups))):
        for t in range(nt):
            for copy in gu_copies(n, t):
                copy.start()
    for d in range(DN_SLOTS):
        for copy in dn_copies(d):
            copy.start()
    ld_copies = [
        remote(ld_all.at[ba], ld_all.at[ba], (ld_s, ld_r), 0, p) for i, p in enumerate(ba_peers)
    ]
    for q in range(PARTS):
        for kx in far:
            own = term(q, kx, False)
            to_side(q, kx).wait_recv()
            e_send[q, kx - 1] = (own + d_recv[q, kx].astype(F32)).astype(BF16)
            to_far(q, kx).start()
    for copy in ld_copies:
        copy.start()

    first, second = expert[0:1, :], expert[1:2, :]
    experts = lax.broadcasted_iota(jnp.int32, (E, toks), 0)
    hit0, hit1 = (first == experts).astype(F32), (second == experts).astype(F32)
    hits = hit0 + hit1
    earlier = (
        lax.broadcasted_iota(jnp.int32, (toks, toks), 0)
        < lax.broadcasted_iota(jnp.int32, (toks, toks), 1)
    ).astype(F32)
    place = jnp.dot(hits.astype(BF16), earlier.astype(BF16), preferred_element_type=F32)
    marked = jnp.where(hits > 0.0, place, -1.0)
    spots = lax.broadcasted_iota(jnp.int32, (CAP, toks), 0)
    picks = jnp.concatenate(
        [(marked[e : e + 1, :].astype(jnp.int32) == spots).astype(F32).astype(BF16) for e in range(E)],
        axis=0,
    )
    seats = lax.broadcasted_iota(jnp.int32, (toks, rows), 1)

    def picked(which, hit):
        seat = which.astype(F32) * (split * CAP) + jnp.sum(hit * place, axis=0, keepdims=True)
        seat = column(seat).astype(jnp.int32)
        found = seats == seat
        for j in range(1, split):
            found = found | (seats == seat + j * CAP)
        return found.astype(F32).astype(BF16)

    pick0[...] = picked(first, hit0)
    pick1[...] = picked(second, hit1)

    def everyone(buf, sems):
        others = buf.at[pl.ds(0, buf.shape[0] - 1)]
        return remote(others, others, sems, 0, partner)

    def here(q, block):
        return q * nx + block

    def dispatch(q, k):
        return remote(
            outgoing.at[q, lax.div(targets[k], split)], x_all.at[here(q, x), ba, :, lane],
            (z_s, z_r), q * (n_ba - 1) + k - 1, {"ba": targets[k]},
        )

    square = jnp.zeros((toks, 1), F32)
    votes = jnp.zeros((E, toks), F32)
    for q in range(PARTS):
        where = slice(q * part, (q + 1) * part)
        delta = term(q, 0, False)
        to_side(q, 0).wait_recv()
        delta = delta + d_recv[q, 0].astype(F32)
        for kx in far:
            to_far(q, kx).wait_recv()
            delta = delta + e_recv[q, kx - 1].astype(F32)
        residual = stream[:, where].astype(F32) + ADAPTER_SCALE * delta
        res[:, where] = residual
        gained = (residual * gain[:, where]).astype(BF16)
        sent = jnp.dot(picks, gained, preferred_element_type=F32)
        outgoing[q] = sent.astype(BF16).reshape(E, CAP, part)
        for k in range(1, n_ba):
            dispatch(q, k).start()
        x_all[here(q, x), ba, :, lane] = outgoing[q, lax.div(ba, split)]
        square = square + jnp.sum(residual * residual, axis=1, keepdims=True)
        votes = votes + lax.dot_general(router[:, where], gained, NT, preferred_element_type=F32)
    stat_all[aa, 0:E] = votes
    stat_all[aa, E : 2 * E] = jnp.broadcast_to(as_row(square), (E, toks))
    stat_copies = [
        remote(stat_all.at[aa], stat_all.at[aa], (stat_s, stat_r), 0, p) for i, p in enumerate(aa_peers)
    ]
    for copy in stat_copies:
        copy.start()
    note_copies = [
        remote(note_all.at[ba], note_all.at[ba], (note_s, note_r), 0, p) for i, p in enumerate(ba_peers)
    ]

    def weigh():
        everyone(stat_all, (stat_s, stat_r)).wait_recv()
        stats = stat_all[0]
        for j in range(1, n_aa):
            stats = stats + stat_all[j]
        inv = lax.rsqrt(stats[E : 2 * E, :] / model_width + EPS)
        note_all[ba, 0:E] = marked
        note_all[ba, E : 2 * E] = inv
        for copy in note_copies:
            copy.start()
        logits = stats[0:E, :] * inv
        own0 = jnp.sum(hit0 * logits, axis=0, keepdims=True)
        own1 = jnp.sum(hit1 * logits, axis=0, keepdims=True)
        weight0[...] = jnp.broadcast_to(column(1.0 / (1.0 + jnp.exp(own1 - own0))), weight0.shape)
        weight1[...] = jnp.broadcast_to(column(1.0 / (1.0 + jnp.exp(own0 - own1))), weight1.shape)

    def read_notes():
        everyone(note_all, (note_s, note_r)).wait_recv()
        everyone(ld_all, (ld_s, ld_r)).wait_recv()
        load = ld_all[0]
        for j in range(1, n_ba):
            load = load + ld_all[j]
        load_ref[...] = load[0:1, 0 : load_ref.shape[1]]
        for s in range(n_ba):
            note = note_all[s, pl.ds(lax.div(ba, split), 1), :]
            seen = note.astype(jnp.int32) == spots
            inv = jnp.sum(jnp.where(seen, note_all[s, E : E + 1, :], 0.0), axis=1, keepdims=True)
            scale[s * CAP : (s + 1) * CAP, :] = jnp.broadcast_to(inv, (CAP, scale.shape[1]))

    def across(q, k, kx):
        block = x_all.at[here(q, x), sources[k], :, lane]
        return remote(block, block, (x_s, x_r), q * (nx - 1) + kx - 1, x_peers[kx - 1])

    def beside(q, k):
        block = x_all.at[here(q, x), sources[k], :, lane]
        return remote(block, block, (c_s, c_r), q, partner)

    def passed(q, kx):
        block = x_all.at[here(q, origins[kx]), :, :, lane]
        return remote(block, block, (f_s, f_r), q * (nx - 1) + kx - 1, partner)

    arrival = list(range(n_ba))

    def forward(q, k):
        if k:
            dispatch(q, k).wait_recv()
        for kx in far:
            across(q, k, kx).start()
        beside(q, k).start()

    def collect(q, kx):
        block = x_all.at[here(q, origins[kx]), :, :, lane]
        i = q * (nx - 1) + kx - 1
        remote(block, block, (x_s, x_r), i, x_peers[kx - 1]).wait_recv()
        passed(q, kx).start()

    steps = len(groups) * nt
    hooks = {}

    def hook(it, fn, *args):
        hooks.setdefault(min(it, steps - 1), []).append(functools.partial(fn, *args))

    def whole(it):
        return it // nt * nt if it > 3 * nt else it

    for q in range(1, PARTS):
        need = groups.index((q, 0)) * nt
        for n, k in enumerate(arrival):
            due = -(-(264 * (q - 1) + 264 * (n + 1) // n_ba + 60) // 100) * nt // 2
            hook(whole(min(max(due, 1), need - 1)), forward, q, k)
    for q in range(PARTS):
        for kx in far:
            need = groups.index((q, kx)) * nt
            floor = groups.index((q, 0)) * nt + (1 if q == 0 else nt)
            hook(max(need - (nt if q else 1), min(floor, need)), collect, q, kx)
    hook((len(groups) - 2) * nt, read_notes)

    def ready(n):
        q, kx = groups[n]
        if kx:
            passed(q, kx).wait_recv()
        else:
            block = x_all.at[here(q, x), :, :, lane]
            remote(block, block, (c_s, c_r), q, partner).wait_recv()

    for k in arrival:
        forward(0, k)
    weigh()
    for n, (q, kx) in enumerate(groups):
        for fn in hooks.get(n * nt, []):
            fn()
        ready(n)

        def fetched(t):
            slot = (n % GU_DEPTH) * nt + t
            for j, buf in enumerate((gw, uw)):
                pltpu.make_async_copy(buf.at[slot], buf.at[slot], gu_s.at[slot, j]).wait()

        def tile(t):
            slot = (n % GU_DEPTH) * nt + t
            lhs = x_all[here(q, origins[kx])].reshape(rows, CORES * part)
            g = jnp.dot(lhs, gw[slot], preferred_element_type=F32)
            u = jnp.dot(lhs, uw[slot], preferred_element_type=F32)
            if n:
                g = gacc[t] + g
                u = uacc[t] + u
            if n == len(groups) - 1:
                factor = scale[:, 0:1]
                g = g * factor
                hidden[:, cols(t * ft, ft)] = (g / (1.0 + jnp.exp(-g)) * (u * factor)).astype(BF16)
            else:
                gacc[t] = g
                uacc[t] = u

        def refill(t):
            if n + GU_DEPTH < len(groups):
                for copy in gu_copies(n + GU_DEPTH, t):
                    copy.start()

        between = [hooks.get(n * nt + j, []) for j in range(1, nt)]
        if nt == 2 and not any(between):
            for stage in (fetched, tile, refill):
                for t in range(nt):
                    stage(t)
        else:
            @pl.loop(0, nt)
            def _(t):
                for j, fns in enumerate(between):
                    if fns:
                        @pl.when(t == j + 1)
                        def _():
                            for fn in fns:
                                fn()
                fetched(t)
                tile(t)
                refill(t)

    def to_partner(q, kx):
        return remote(ys.at[q, kx], c1.at[q, kx], (p_s, p_r), q * nx + kx, partner)

    def to_chip(q, kx, k):
        i = (q * (nx - 1) + kx - 1) * n_ba + k
        return remote(
            xs.at[q, kx - 1, targets[k]], c2.at[q, kx - 1, targets[k]], (q_s, q_r), i, x_peers[kx - 1]
        )

    def home(q, k):
        return remote(
            bs.at[q, k - 1], ret.at[q, ba], (b_s, b_r), q, {"ba": targets[k]}
        )

    def give(q, k):
        to = targets[k]
        whole = yown[q, to]
        for kx in far:
            to_chip(q, kx, k).wait_recv()
            whole = whole + c2[q, kx - 1, to].astype(F32)
        if k:
            bs[q, k - 1] = whole.astype(BF16)
            home(q, k).start()
        else:
            ret[q, ba] = whole.astype(BF16)

    def leave(q):
        where = pl.ds(q * part, part)
        return pltpu.make_async_copy(out.at[:, where], out_hbm.at[:, where], out_s.at[q])

    def blend(q):
        remote(bs.at[q], bs.at[q], (b_s, b_r), q, partner).wait_recv()
        where = slice(q * part, (q + 1) * part)
        back = ret[q].reshape(rows, part)
        mixed = weight0[:, 0:1] * jnp.dot(pick0[...], back, preferred_element_type=F32)
        mixed = mixed + weight1[:, 0:1] * jnp.dot(pick1[...], back, preferred_element_type=F32)
        out[:, where] = (res[:, where] + mixed).astype(BF16)
        leave(q).start()

    order = list(range(1, n_ba)) + [0]
    last = len(chunks) - 1
    gives = {}
    for q in range(PARTS):
        for n, k in enumerate(order):
            due = -(-(540 + 420 * q + 52 * n * 8 // n_ba) // 160) - 1
            due = max(due * nx // 2, (q + 1) * nx)
            gives.setdefault(min(due, last), []).append((q, k))

    def finish(q, kx):
        to_partner(q, kx).wait_recv()
        if kx:
            for k in order:
                to = targets[k]
                xs[q, kx - 1, to] = (yfar[kx - 1, to] + c1[q, kx, to].astype(F32)).astype(BF16)
                to_chip(q, kx, k).start()
        else:
            yown[q] = yown[q] + c1[q, kx].astype(F32)

    late = None
    for d, (q, kx) in enumerate(chunks):
        for copy in dn_copies(d):
            copy.wait()
        slot = d % DN_SLOTS
        y = [jnp.dot(hidden[...], dw[slot, i], preferred_element_type=F32) for i in range(CORES)]
        ys[q, kx] = y[1].astype(BF16).reshape(n_ba, CAP, part)
        to_partner(q, kx).start()
        if kx:
            yfar[kx - 1] = y[0].reshape(n_ba, CAP, part)
        else:
            yown[q] = y[0].reshape(n_ba, CAP, part)
        if d + DN_SLOTS < len(chunks):
            for copy in dn_copies(d + DN_SLOTS):
                copy.start()
        if late is not None:
            finish(*late)
        late = (q, kx)
        if d == 0 or d == last:
            finish(q, kx)
            late = None
        done = set()
        for qq, k in gives.get(d, []):
            if d == last and qq > 1 and qq - 2 not in done:
                blend(qq - 2)
                done.add(qq - 2)
            give(qq, k)
    for q in range(PARTS):
        if q not in done:
            blend(q)

    for buf, sems in ((stat_all, (stat_s, stat_r)), (note_all, (note_s, note_r)), (ld_all, (ld_s, ld_r))):
        everyone(buf, sems).wait_send()
    local_part = x_all.at[pl.ds(0, PARTS), :, :, pl.ds(0, part)]
    passes = x_all.at[pl.ds(0, PARTS * (nx - 1)), :, :, pl.ds(0, part)]
    for buf, sems in (
        (bs, (z_s, z_r)), (bs, (b_s, b_r)), (local_part, (c_s, c_r)), (passes, (x_s, x_r)),
        (passes, (f_s, f_r)), (xs, (q_s, q_r)), (ys, (p_s, p_r)), (d_send, (d_s, d_r)),
        (e_send, (e_s, e_r)),
    ):
        remote(buf, buf, sems, 0, partner).wait_send()
    for q in range(PARTS):
        leave(q).wait()


def shards(
    head_outputs,
    stream,
    adapter_down_factors,
    adapter_up_factors,
    norm_gain_vector,
    router_matrix,
    token_adapter_index,
    token_expert_index,
    gate_weight,
    up_weight,
    down_weight,
):
    toks, model_width = head_outputs.shape
    n_aa, n_ba = lax.axis_size("aa"), lax.axis_size("ba")
    nx = n_aa // CORES
    held = adapter_down_factors.shape[1]
    ff = gate_weight.shape[2]
    width = model_width // n_aa
    part = width // PARTS
    rows = n_ba * CAP
    nt = 2 if ff % 512 == 0 else ff // 128
    dma = pltpu.SemaphoreType.DMA
    vmem = pltpu.VMEM
    far = max(nx - 1, 1)

    def sems(n):
        return [dma((1,)), dma((max(n, 1),))]

    mixed, load = pl.pallas_call(
        functools.partial(layer, n_aa, n_ba, nt),
        out_shape=(
            jax.ShapeDtypeStruct((toks, width), BF16),
            jax.ShapeDtypeStruct((1, held // ADAPTER_RANK), F32),
        ),
        in_specs=[pl.BlockSpec(memory_space=pl.ANY)] * 11,
        out_specs=(pl.BlockSpec(memory_space=pl.ANY), pl.BlockSpec(memory_space=pltpu.VMEM)),
        scratch_shapes=[
            vmem((toks, model_width), BF16),
            vmem((toks, width), BF16),
            vmem((model_width, held), BF16),
            vmem((held, model_width), BF16),
            vmem((1, width), F32),
            vmem((E, width), BF16),
            vmem((1, toks), jnp.int32),
            vmem((2, toks), jnp.int32),
            vmem((PARTS, nx, toks, part), BF16),
            vmem((PARTS, nx, toks, part), BF16),
            vmem((PARTS, far, toks, part), BF16),
            vmem((PARTS, far, toks, part), BF16),
            vmem((n_aa, 2 * E, toks), F32),
            vmem((n_ba, 2 * E, toks), F32),
            vmem((n_ba, 8, held), F32),
            vmem((toks, width), F32),
            vmem((PARTS, E, CAP, part), BF16),
            vmem((rows, 128), F32),
            vmem((toks, rows), BF16),
            vmem((toks, rows), BF16),
            vmem((toks, 128), F32),
            vmem((toks, 128), F32),
            vmem((toks, width), BF16),
            vmem((PARTS * nx, n_ba, CAP, CORES * part), BF16),
            vmem((nt, rows, ff // nt), F32),
            vmem((nt, rows, ff // nt), F32),
            vmem((rows, ff), BF16),
            vmem((GU_DEPTH * nt, CORES * part, ff // nt), BF16),
            vmem((GU_DEPTH * nt, CORES * part, ff // nt), BF16),
            vmem((DN_SLOTS, CORES, ff, part), BF16),
            vmem((PARTS, nx, n_ba, CAP, part), BF16),
            vmem((PARTS, nx, n_ba, CAP, part), BF16),
            vmem((PARTS, n_ba, CAP, part), F32),
            vmem((far, n_ba, CAP, part), F32),
            vmem((PARTS, far, n_ba, CAP, part), BF16),
            vmem((PARTS, far, n_ba, CAP, part), BF16),
            vmem((PARTS, n_ba - 1, CAP, part), BF16),
            vmem((PARTS, n_ba, CAP, part), BF16),
            dma((8,)),
            dma((GU_DEPTH * nt, 2)),
            dma((DN_SLOTS, CORES)),
            dma((PARTS,)),
        ]
        + sems(PARTS * nx)
        + sems(PARTS * (nx - 1))
        + sems(1) * 3
        + sems(PARTS * (n_ba - 1))
        + sems(PARTS * (nx - 1))
        + sems(PARTS)
        + sems(PARTS * (nx - 1))
        + sems(PARTS * nx)
        + sems(PARTS * n_ba * (nx - 1))
        + sems(PARTS),
        compiler_params=pltpu.CompilerParams(
            collective_id=0, has_side_effects=True, vmem_limit_bytes=67043328
        ),
        name="layer",
    )(
        head_outputs, stream, adapter_down_factors, adapter_up_factors,
        norm_gain_vector[None, :], router_matrix.T, token_adapter_index[None, :],
        token_expert_index.T, gate_weight, up_weight, down_weight,
    )
    return (mixed, load.reshape(held // ADAPTER_RANK))


def solution(mesh):
    in_specs = (
        P("ba", None),
        P("ba", None),
        P(None, "aa"),
        P("aa", None),
        P(),
        P(),
        P("ba"),
        P("ba", None),
        P("ba", None, "aa"),
        P("ba", None, "aa"),
        P("ba", "aa", None),
    )
    out_specs = (P("ba", "aa"), P("aa"))
    return jax.shard_map(shards, mesh=mesh, in_specs=in_specs, out_specs=out_specs, check_vma=False)
```
